32 devices in a mesh: lon: 2 (over x), lat: 4 (over y, core), head: 4 (over z).
Axes of the slice: x: 2, y: 2, z: 4, core: 2. Of those that a mesh axis runs over, the one named last changes fastest.
Arguments:
- features: bfloat16 [8, 24, 24, 384], P(None, 'lat', 'lon'), may hold values from -6 to 6
- attend_weight: bfloat16 [3, 384, 384], P(None, None, 'head'), may hold values from -0.3125 to 0.3125
- output_weight: bfloat16 [384, 384], P('head'), may hold values from -0.3125 to 0.3125
- bias_table: float32 [64, 12, 3312], P(None, 'head'), may hold values from -3 to 304
- bias_type: int32 [4, 4], P(None, 'lat'), may hold values from 0 to 63
- window_shift: int32 [1], replicated, may hold values from 1 to 11
- grad_out: bfloat16 [8, 24, 24, 384], P(None, 'lat', 'lon'), may hold values from -6 to 6
Outputs:
- feature_grad: bfloat16 [8, 24, 24, 384], P(None, 'lat', 'lon', 'head')
- attend_grad: float32 [3, 384, 384], P(None, None, 'head')
- output_grad: float32 [384, 384], P('head')
- bias_grad: float32 [64, 12, 3312], P(None, 'head')
The draws below stay inside these ranges and needn't reach their ends.
All inputs are finite; a program needn't handle non-finite values.
Results may differ from the reference program's by a relative error of at most 0.01.
Values may be sent and summed in bfloat16 or wider, within the bound.
A program may use at most 128 MiB of HBM per device.

```python
import jax
import jax.numpy as jnp
import numpy as np
from jax import lax

D = 384
HEADS = 12
TYPES = 64
WIN_LEVEL = 2
WIN_LAT = 6
WIN_LON = 12
REL_COUNT = 3312
LEVELS = 8
LAT = 24
LON = 24
LEVEL_WINS = 4
LAT_WINS = 4
N_HEAD = 4


def draw_bias_table(key, part):
    base_key = jax.random.fold_in(key, 11)
    first_key = jax.random.fold_in(base_key, 0)
    table = jnp.clip(jax.random.normal(first_key, (TYPES, HEADS, REL_COUNT), jnp.float32), -3.0, 3.0)
    return table


def with_ends(values, key, smallest, top_value):
    spot = [jax.random.randint(jax.random.fold_in(key, axis), (), 0, length) for axis, length in enumerate(values.shape)]
    main_axis = values.shape.index(max(values.shape))
    next_to = spot[:main_axis] + [(spot[main_axis] + 1) % values.shape[main_axis]] + spot[main_axis + 1:]
    return values.at[tuple(spot)].set(smallest).at[tuple(next_to)].set(top_value)


def levels(rng, extent, shards, least, high):
    gain, own = 1.0, jax.random.fold_in(rng, 6)
    for dim, shards_of in shards:
        heights = jnp.exp(jax.random.uniform(jax.random.fold_in(own, dim), (shards_of,), jnp.float32, least / len(shards), high / len(shards)))
        gain = gain * jnp.repeat(heights, extent[dim] // shards_of).reshape([-1 if axis == dim else 1 for axis in range(len(extent))])
    return gain


def centred(own_key, dims, width, most, cuts=(), held_as=jnp.bfloat16):
    gain = levels(own_key, dims, cuts, -0.22, 0.18) if cuts else 1.0
    entries = jax.random.normal(own_key, dims, jnp.float32) * width * gain
    return jnp.minimum(jnp.maximum(entries, -most), most).astype(held_as)


def setup_inputs(seed: int = 0) -> dict:
    seeds = jax.random.split(jax.random.key(seed), 8)
    return {
        "features": centred(seeds[0], (LEVELS, LAT, LON, D), 1.0, 6.0, ((1, 4), (2, 2))),
        "attend_weight": centred(seeds[1], (3, D, D), D ** -0.5, 0.3125, ((2, 4),)),
        "output_weight": centred(seeds[2], (D, D), D ** -0.5, 0.3125, ((0, 4),)),
        "bias_table": draw_bias_table(jax.random.fold_in(seeds[7], 71), 0),
        "bias_type": with_ends(jax.random.randint(seeds[4], (LEVEL_WINS, LAT_WINS), 0, TYPES), jax.random.fold_in(seeds[4], 1), 0, TYPES - 1).astype(jnp.int32),
        "window_shift": jax.random.randint(seeds[5], (1,), 1, WIN_LON).astype(jnp.int32),
        "grad_out": centred(seeds[6], (LEVELS, LAT, LON, D), 1.0, 6.0, ((1, 4), (2, 2))),
    }


def relative_index(win_level, win_lat, win_lon):
    level_pos, lat_pos, lon_pos = np.meshgrid(np.arange(win_level), np.arange(win_lat), np.arange(win_lon), indexing="ij")
    level_pos = level_pos.reshape(-1)
    lat_pos = lat_pos.reshape(-1)
    lon_pos = lon_pos.reshape(-1)
    pair_level = level_pos[:, None] * win_level + level_pos[None, :]
    pair_lat = lat_pos[:, None] * win_lat + lat_pos[None, :]
    offset_lon = lon_pos[:, None] - lon_pos[None, :] + win_lon - 1
    combined = (pair_level * win_lat * win_lat + pair_lat) * (2 * win_lon - 1) + offset_lon
    return jnp.asarray(combined.reshape(-1).astype(np.int32))


def halve(values):
    return lax.optimization_barrier(values.astype(jnp.bfloat16)).astype(jnp.float32)


def attend_backward(tokens, grad_rows, window_types, attend_weight, output_weight, bias_table, relation):
    outer_count, inner_count, win_tokens, model_width = tokens.shape
    head_count = bias_table.shape[1]
    head_size = attend_weight.shape[2] // head_count
    scaling = head_size ** -0.5
    tokens_full = tokens.astype(jnp.float32)
    grad_full = grad_rows.astype(jnp.float32)
    projected = halve(jnp.einsum("abnd,cdk->cabnk", tokens_full, attend_weight.astype(jnp.float32)))
    split = projected.reshape(3, outer_count, inner_count, win_tokens, head_count, head_size)
    queries, key_rows, values = split[0], split[1], split[2]
    table_rows = jnp.take(bias_table, window_types, axis=0)
    bias_full = jnp.take(table_rows, relation, axis=2).reshape(outer_count, head_count, win_tokens, win_tokens)
    scores = jnp.einsum("abihe,abjhe->abhij", queries, key_rows) * scaling + bias_full[:, None]
    softened = jax.nn.softmax(scores, axis=-1)
    softened_half = halve(softened)
    attended = halve(jnp.einsum("abhij,abjhe->abihe", softened_half, values))
    grad_attended = halve(jnp.einsum("abnd,kd->abnk", grad_full, output_weight.astype(jnp.float32)))
    grad_heads = grad_attended.reshape(outer_count, inner_count, win_tokens, head_count, head_size)
    grad_values = halve(jnp.einsum("abhij,abihe->abjhe", softened_half, grad_heads))
    grad_softened = jnp.einsum("abihe,abjhe->abhij", grad_heads, values)
    grad_scores = softened * (grad_softened - jnp.sum(softened * grad_softened, axis=-1, keepdims=True))
    grad_scores_half = halve(grad_scores)
    grad_queries = halve(jnp.einsum("abhij,abjhe->abihe", grad_scores_half, key_rows) * scaling)
    grad_keys = halve(jnp.einsum("abhij,abihe->abjhe", grad_scores_half, queries) * scaling)
    grad_projected = jnp.stack([grad_queries, grad_keys, grad_values]).reshape(3, outer_count, inner_count, win_tokens, head_count * head_size)
    attended = attended.reshape(outer_count, inner_count, win_tokens, head_count * head_size)
    return attended, grad_projected, grad_scores


def reference(features, attend_weight, output_weight, bias_table, bias_type, window_shift, grad_out):
    offset = window_shift[0]
    rolled = jnp.roll(features, -offset, axis=2)
    rolled_grad = jnp.roll(grad_out, -offset, axis=2)
    relation = relative_index(WIN_LEVEL, WIN_LAT, WIN_LON)
    lon_wins = LON // WIN_LON
    level_wins = LEVELS // WIN_LEVEL
    win_tokens = WIN_LEVEL * WIN_LAT * WIN_LON
    head_count = bias_table.shape[1]
    rel_total = bias_table.shape[2]
    group_cols = D // N_HEAD

    def to_windows(band):
        shaped = band.reshape(level_wins, WIN_LEVEL, WIN_LAT, lon_wins, WIN_LON, D)
        return shaped.transpose(0, 3, 1, 2, 4, 5).reshape(level_wins, lon_wins, win_tokens, D)

    def from_windows(windows):
        shaped = windows.reshape(level_wins, lon_wins, WIN_LEVEL, WIN_LAT, WIN_LON, D)
        return shaped.transpose(0, 2, 3, 1, 4, 5).reshape(LEVELS, WIN_LAT, LON, D)

    def band_step(totals, band_index):
        grad_attend, grad_output, grad_bias = totals
        band_start = band_index * WIN_LAT
        tokens = to_windows(lax.dynamic_slice_in_dim(rolled, band_start, WIN_LAT, 1))
        grad_rows = to_windows(lax.dynamic_slice_in_dim(rolled_grad, band_start, WIN_LAT, 1))
        window_types = lax.dynamic_slice_in_dim(bias_type, band_index, 1, 1)[:, 0].astype(jnp.int32)
        attended, grad_projected, grad_scores = attend_backward(tokens, grad_rows, window_types, attend_weight, output_weight, bias_table, relation)
        tokens_full = tokens.astype(jnp.float32)
        grad_attend = grad_attend + jnp.einsum("abnd,cabnk->cdk", tokens_full, grad_projected)
        grad_output = grad_output + jnp.einsum("abnk,abnd->kd", attended, grad_rows.astype(jnp.float32))
        summed_scores = jnp.sum(grad_scores, axis=1).reshape(-1)
        segment_ids = (window_types[:, None, None] * head_count * rel_total + jnp.arange(head_count, dtype=jnp.int32)[None, :, None] * rel_total + relation[None, None, :]).reshape(-1)
        grad_bias = grad_bias + jax.ops.segment_sum(summed_scores, segment_ids, num_segments=bias_table.shape[0] * head_count * rel_total).reshape(bias_table.shape)
        grouped = grad_projected.reshape(3, level_wins, lon_wins, win_tokens, N_HEAD, group_cols)
        weight_grouped = attend_weight.astype(jnp.float32).reshape(3, D, N_HEAD, group_cols)
        pieces = halve(jnp.einsum("cabngk,cdgk->gabnd", grouped, weight_grouped))
        band_grad = from_windows(jnp.sum(pieces, axis=0)).astype(jnp.bfloat16)
        return (grad_attend, grad_output, grad_bias), band_grad

    start_totals = (jnp.zeros((3, D, D), jnp.float32), jnp.zeros((D, D), jnp.float32), jnp.zeros(bias_table.shape, jnp.float32))
    totals, bands = lax.scan(band_step, start_totals, jnp.arange(LAT // WIN_LAT, dtype=jnp.int32))
    grid_grad = bands.transpose(1, 0, 2, 3, 4).reshape(LEVELS, LAT, LON, D)
    feature_grad = jnp.roll(grid_grad, offset, axis=2)
    return feature_grad, totals[0], totals[1], totals[2]
```

```python
import functools

import jax
import jax.numpy as jnp
from jax import lax
from jax.experimental import pallas as pl
from jax.experimental.pallas import tpu as pltpu
from jax.sharding import PartitionSpec as P

WIN_LEVEL = 2
WIN_LAT = 6
WIN_LON = 12
ROWS = WIN_LEVEL * WIN_LAT
HALF = WIN_LON // 2
SPAN = 2 * WIN_LON - 1
PAD = 16
TOK = ROWS * PAD
F32 = jnp.float32
BF16 = jnp.bfloat16


def from_behind(x, axis, by):
    count = lax.axis_size(axis)
    return lax.ppermute(x, axis, [(i, (i + by) % count) for i in range(count)])


def dot(a, b, dims):
    return lax.dot_general(a, b, (dims, ((), ())), preferred_element_type=F32)


NN = ((1,), (0,))
NT = ((1,), (1,))
TN = ((0,), (0,))


def use_neighbour(shift, col):
    first = jnp.where(shift <= HALF, 0, shift)
    return (col >= first) & (col < jnp.where(shift <= HALF, shift, WIN_LON))


def block_kernel(heads, shift_ref, type_ref, x_ref, g_ref, low_ref, high_ref, aw_ref, ow_ref, table_ref,
                 piece_ref, grad_aw_ref, grad_ow_ref, grad_bias_ref,
                 xs, gs, proj, gproj, att, bias_a, bias_b, rel, table, sems):
    shift = shift_ref[0]
    wins = table.shape[0]
    width = x_ref.shape[-1]
    inner = aw_ref.shape[2]
    size = inner // heads
    part = WIN_LAT * SPAN
    copies = [
        pltpu.make_async_copy(table_ref.at[type_ref[w, 0]], table.at[w], sems.at[w]) for w in range(wins)
    ]
    for copy in copies:
        copy.start()

    lines = wins * ROWS
    col = lax.broadcasted_iota(jnp.int32, (lines, WIN_LON, width), 1)
    taken = use_neighbour(shift, col)
    for src, dst, n in ((x_ref, xs, 0), (g_ref, gs, 1)):
        near = jnp.concatenate([low_ref[n].astype(F32), high_ref[n].astype(F32)], axis=1)
        picked = jnp.where(taken, near, src[...].astype(F32))
        full = jnp.concatenate([picked, jnp.zeros((lines, PAD - WIN_LON, width), F32)], axis=1)
        dst[...] = full.astype(BF16).reshape(lines * PAD, width)
    tokens = xs[...]
    grads = gs[...]
    for c in range(3):
        proj[c] = dot(tokens, aw_ref[c], NN).astype(BF16)
    proj[3] = dot(grads, ow_ref[...], NT).astype(BF16)

    for copy in copies:
        copy.wait()
    rel[...] = jnp.zeros_like(rel)
    for w in range(wins):
        for k in range(WIN_LEVEL * WIN_LEVEL * WIN_LAT):
            zi, zj, ai = k // (WIN_LEVEL * WIN_LAT), k // WIN_LAT % WIN_LEVEL, k % WIN_LAT
            rel[zi * WIN_LAT + ai, w * heads:(w + 1) * heads, zj * part:(zj + 1) * part] = table[
                w, :, k * part:(k + 1) * part
            ]
    lanes = rel.shape[2]
    row = lax.broadcasted_iota(jnp.int32, (lanes, TOK), 0)
    key = lax.broadcasted_iota(jnp.int32, (lanes, TOK), 1)
    slot = key % PAD
    pos = slot + WIN_LON - shift
    pos = jnp.where(pos >= WIN_LON, pos - WIN_LON, pos)
    hit = (row == key // PAD * SPAN + WIN_LON - 1 - pos) & (slot < WIN_LON)
    spread = jnp.where(hit, 1.0, 0.0).astype(BF16)
    unused = jnp.where(lax.broadcasted_iota(jnp.int32, (1, TOK), 1) % PAD < WIN_LON, 0.0, -1e30)
    group = PAD
    flat = rel[...].reshape(ROWS * group, lanes)
    for c in range(PAD):
        if c < WIN_LON:
            place = lax.rem(c + WIN_LON - shift, WIN_LON)
            moved = pltpu.roll(flat, lanes - place, 1)
            one = moved.astype(BF16)
            rest = moved - one.astype(F32)
            two = rest.astype(BF16)
            three = (rest - two.astype(F32)).astype(BF16)
            out = dot(one, spread, NN) + dot(two, spread, NN) + dot(three, spread, NN) + unused
        else:
            out = jnp.zeros((ROWS * group, TOK), F32)
        for p in range(ROWS):
            base = (p * PAD + c) * group
            bias_a[base:base + group, :] = out[p * group:(p + 1) * group, :128]
            bias_b[base:base + group, :TOK - 128] = out[p * group:(p + 1) * group, 128:]

    scaling = size ** -0.5
    lane = lax.broadcasted_iota(jnp.int32, (TOK, inner), 1) // size
    for w in range(wins):
        span = slice(w * TOK, (w + 1) * TOK)
        q, k, v, ga = proj[0, span], proj[1, span], proj[2, span], proj[3, span]
        sums = [None] * 4
        for h in range(heads):
            e = w * heads + h
            mine = (lane == h).astype(BF16)
            qh, kh, vh, gah = q * mine, k * mine, v * mine, ga * mine
            rows = pl.ds(e, TOK, stride=group)
            bias = jnp.concatenate([bias_a[rows, :], bias_b[rows, :][:, :TOK - 128]], axis=1)
            scores = dot(qh, k, NT) * scaling + bias
            top = jnp.max(scores, axis=1, keepdims=True)
            raised = jnp.exp(scores - top)
            soft = raised * (1.0 / jnp.sum(raised, axis=1, keepdims=True))
            half = soft.astype(BF16)
            grad_soft = dot(gah, v, NT)
            both = soft * grad_soft
            grad_scores = both - soft * jnp.sum(both, axis=1, keepdims=True)
            bias_a[rows, :] = grad_scores[:, :128]
            bias_b[rows, :] = jnp.concatenate(
                [grad_scores[:, 128:], jnp.zeros((TOK, 256 - TOK), F32)], axis=1
            )
            gsh = grad_scores.astype(BF16)
            terms = (dot(half, vh, NN), dot(gsh, kh, NN), dot(gsh, qh, TN), dot(half, gah, TN))
            sums = [t if s is None else s + t for s, t in zip(sums, terms)]
        att[span] = sums[0].astype(BF16)
        gproj[0, span] = (sums[1] * scaling).astype(BF16)
        gproj[1, span] = (sums[2] * scaling).astype(BF16)
        gproj[2, span] = sums[3].astype(BF16)

    chunks, chunk = piece_ref.shape[0], piece_ref.shape[-1]
    for n in range(chunks):
        cols = slice(n * chunk, (n + 1) * chunk)
        total = sum(dot(gproj[c], aw_ref[c, cols, :], NT) for c in range(3))
        piece_ref[n] = total.reshape(lines, PAD, chunk)[:, :WIN_LON].astype(BF16)
    for c in range(3):
        grad_aw_ref[c] = dot(tokens, gproj[c], TN)
    grad_ow_ref[...] = dot(att[...], grads, TN)

    folded = jnp.zeros((ROWS * group, lanes), F32)
    for c in range(WIN_LON):
        place = lax.rem(c + WIN_LON - shift, WIN_LON)
        parts = []
        for p in range(ROWS):
            base = (p * PAD + c) * group
            parts.append(
                jnp.concatenate(
                    [bias_a[base:base + group, :], bias_b[base:base + group, :][:, :TOK - 128]], axis=1
                )
            )
        got = jnp.concatenate(parts, axis=0)
        one = got.astype(BF16)
        two = (got - one.astype(F32)).astype(BF16)
        folded = folded + pltpu.roll(dot(one, spread, NT) + dot(two, spread, NT), place, 1)
    rel[...] = folded.reshape(ROWS, group, lanes)
    for w in range(wins):
        for k in range(WIN_LEVEL * WIN_LEVEL * WIN_LAT):
            zi, zj, ai = k // (WIN_LEVEL * WIN_LAT), k // WIN_LAT % WIN_LEVEL, k % WIN_LAT
            grad_bias_ref[w, :, k * part:(k + 1) * part] = rel[
                zi * WIN_LAT + ai, w * heads:(w + 1) * heads, zj * part:(zj + 1) * part
            ]


def block_backward(features, grad_out, low, high, attend_weight, output_weight, bias_table, bias_type, shift):
    levels, lat_rows, lon_cols, width = features.shape
    heads, rel_total = bias_table.shape[1:]
    inner = attend_weight.shape[2]
    wins = levels // WIN_LEVEL
    lines = wins * ROWS
    chunks = lax.axis_size("head")
    vmem = pl.BlockSpec(memory_space=pltpu.VMEM)
    smem = pl.BlockSpec(memory_space=pltpu.SMEM)
    lanes = -(-ROWS * SPAN // 128) * 128
    total = lines * PAD
    return pl.pallas_call(
        functools.partial(block_kernel, heads),
        out_shape=(
            jax.ShapeDtypeStruct((chunks, lines, WIN_LON, width // chunks), BF16),
            jax.ShapeDtypeStruct(attend_weight.shape, F32),
            jax.ShapeDtypeStruct(output_weight.shape, F32),
            jax.ShapeDtypeStruct((wins, heads, rel_total), F32),
        ),
        in_specs=[smem, smem, vmem, vmem, vmem, vmem, vmem, vmem, pl.BlockSpec(memory_space=pl.ANY)],
        out_specs=(vmem, vmem, vmem, vmem),
        scratch_shapes=[
            pltpu.VMEM((total, width), BF16),
            pltpu.VMEM((total, width), BF16),
            pltpu.VMEM((4, total, inner), BF16),
            pltpu.VMEM((3, total, inner), BF16),
            pltpu.VMEM((total, inner), BF16),
            pltpu.VMEM((TOK * PAD, 128), F32),
            pltpu.VMEM((TOK * PAD, 128), F32),
            pltpu.VMEM((ROWS, PAD, lanes), F32),
            pltpu.VMEM((wins, heads, rel_total), F32),
            pltpu.SemaphoreType.DMA((wins,)),
        ],
        compiler_params=pltpu.CompilerParams(vmem_limit_bytes=50 * 1024 * 1024),
        cost_estimate=pl.CostEstimate(flops=10**9, bytes_accessed=10**7, transcendentals=10**6),
    )(
        shift,
        bias_type,
        features.reshape(lines, lon_cols, width),
        grad_out.reshape(lines, lon_cols, width),
        low,
        high,
        attend_weight,
        output_weight,
        bias_table,
    )


def swap_columns(low, high, shift):
    if lax.axis_size("lon") <= 2:
        got = from_behind(jnp.where(shift <= HALF, low, high), "lon", 1)
        return got, got
    return from_behind(low, "lon", -1), from_behind(high, "lon", 1)


def per_device(features, attend_weight, output_weight, bias_table, bias_type, window_shift, grad_out):
    shift = window_shift[0]
    levels, lat_rows, lon_cols, width = features.shape
    stacked = jnp.stack((features, grad_out)).reshape(2, levels * lat_rows, lon_cols, width)
    low, high = swap_columns(stacked[:, :, :HALF], stacked[:, :, HALF:], shift)
    pieces, grad_attend, grad_output, grad_bias = block_backward(
        features, grad_out, low, high, attend_weight, output_weight, bias_table, bias_type, window_shift
    )
    summed = lax.psum_scatter(pieces, "head", scatter_dimension=0, tiled=False)
    low, high = swap_columns(summed[:, :HALF], summed[:, HALF:], shift)
    taken = use_neighbour(shift, jnp.arange(lon_cols))[None, :, None]
    feature_grad = jnp.where(taken, jnp.concatenate((low, high), axis=1), summed)
    feature_grad = feature_grad.reshape(levels, lat_rows, lon_cols, -1)
    attend_grad, output_grad = lax.psum((grad_attend, grad_output), ("lon", "lat"))
    parts = lax.all_gather(grad_bias, ("lon", "lat")).reshape(-1, *bias_table.shape[1:])
    types = lax.all_gather(bias_type[:, 0], ("lon", "lat")).reshape(-1)
    selector = (types[:, None] == jnp.arange(bias_table.shape[0], dtype=jnp.int32)[None, :]).astype(F32)
    bias_grad = jnp.einsum("at,ahr->thr", selector, parts, precision=lax.Precision.HIGHEST)
    return (feature_grad, attend_grad, output_grad, bias_grad)


def solution(mesh):
    placed = (
        P(None, "lat", "lon", None),
        P(None, None, "head"),
        P("head", None),
        P(None, "head", None),
        P(None, "lat"),
        P(),
        P(None, "lat", "lon", None),
    )
    return jax.shard_map(
        per_device,
        mesh=mesh,
        in_specs=placed,
        out_specs=(
            P(None, "lat", "lon", "head"),
            P(None, None, "head"),
            P("head", None),
            P(None, "head", None),
        ),
        check_vma=False,
    )
```

```python
import functools

import jax
import jax.numpy as jnp
from jax import lax
from jax.experimental import pallas as pl
from jax.experimental.pallas import tpu as pltpu
from jax.sharding import PartitionSpec as P

WIN_LEVEL = 2
WIN_LAT = 6
WIN_LON = 12
ROWS = WIN_LEVEL * WIN_LAT
HALF = WIN_LON // 2
SPAN = 2 * WIN_LON - 1
PAD = 16
TOK = ROWS * PAD
F32 = jnp.float32
BF16 = jnp.bfloat16


def from_behind(x, axis, by):
    count = lax.axis_size(axis)
    return lax.ppermute(x, axis, [(i, (i + by) % count) for i in range(count)])


def dot(a, b, dims):
    return lax.dot_general(a, b, (dims, ((), ())), preferred_element_type=F32)


NN = ((1,), (0,))
NT = ((1,), (1,))
TN = ((0,), (0,))


def use_neighbour(shift, col):
    first = jnp.where(shift <= HALF, 0, shift)
    return (col >= first) & (col < jnp.where(shift <= HALF, shift, WIN_LON))


def block_kernel(heads, shift_ref, type_ref, x_ref, g_ref, low_ref, high_ref, aw_ref, ow_ref, table_ref,
                 piece_ref, grad_w_ref, grad_bias_ref, kinds_ref,
                 xs, gs, proj, gproj, att, bias_a, bias_b, rel, table, line, piece, sems):
    shift = shift_ref[0]
    wins = table.shape[0]
    width = x_ref.shape[-1]
    inner = aw_ref.shape[2]
    size = inner // heads
    part = WIN_LAT * SPAN
    copies = [
        pltpu.make_async_copy(table_ref.at[type_ref[w, 0]], table.at[w], sems.at[w]) for w in range(wins)
    ]
    for copy in copies:
        copy.start()

    lines = wins * ROWS
    col = lax.broadcasted_iota(jnp.int32, (lines, WIN_LON, width), 1)
    taken = use_neighbour(shift, col)
    for src, dst, n in ((x_ref, xs, 0), (g_ref, gs, 1)):
        near = jnp.concatenate([low_ref[n].astype(F32), high_ref[n].astype(F32)], axis=1)
        picked = jnp.where(taken, near, src[...].astype(F32))
        full = jnp.concatenate([picked, jnp.zeros((lines, PAD - WIN_LON, width), F32)], axis=1)
        dst[...] = full.astype(BF16).reshape(lines * PAD, width)
    tokens = xs[...]
    grads = gs[...]
    for c in range(3):
        proj[c] = dot(tokens, aw_ref[c], NN).astype(BF16)
    proj[3] = dot(grads, ow_ref[...], NT).astype(BF16)

    for copy in copies:
        copy.wait()
    rel[...] = jnp.zeros_like(rel)
    line[...] = jnp.zeros_like(line)
    kinds_ref[...] = jnp.full_like(kinds_ref, -1)
    for w in range(wins):
        line[w * heads:(w + 1) * heads, :table.shape[2]] = table[w]
        kinds_ref[w * heads:(w + 1) * heads, :] = jnp.full((heads, kinds_ref.shape[1]), type_ref[w, 0], jnp.int32)
    for k in range(WIN_LEVEL * WIN_LEVEL * WIN_LAT):
        zi, zj, ai = k // (WIN_LEVEL * WIN_LAT), k // WIN_LAT % WIN_LEVEL, k % WIN_LAT
        rel[zi * WIN_LAT + ai, :, zj * part:(zj + 1) * part] = line[:, k * part:(k + 1) * part]
    lanes = rel.shape[2]
    row = lax.broadcasted_iota(jnp.int32, (lanes, TOK), 0)
    key = lax.broadcasted_iota(jnp.int32, (lanes, TOK), 1)
    slot = key % PAD
    pos = slot + WIN_LON - shift
    pos = jnp.where(pos >= WIN_LON, pos - WIN_LON, pos)
    hit = (row == key // PAD * SPAN + WIN_LON - 1 - pos) & (slot < WIN_LON)
    spread = jnp.where(hit, 1.0, 0.0).astype(BF16)
    unused = jnp.where(lax.broadcasted_iota(jnp.int32, (1, TOK), 1) % PAD < WIN_LON, 0.0, -1e30)
    group = PAD
    flat = rel[...].reshape(ROWS * group, lanes)
    for c in range(PAD):
        if c < WIN_LON:
            place = lax.rem(c + WIN_LON - shift, WIN_LON)
            moved = pltpu.roll(flat, lanes - place, 1)
            one = moved.astype(BF16)
            rest = moved - one.astype(F32)
            two = rest.astype(BF16)
            three = (rest - two.astype(F32)).astype(BF16)
            out = dot(one, spread, NN) + dot(two, spread, NN) + dot(three, spread, NN) + unused
        else:
            out = jnp.zeros((ROWS * group, TOK), F32)
        for p in range(ROWS):
            base = (p * PAD + c) * group
            bias_a[base:base + group, :] = out[p * group:(p + 1) * group, :128]
            bias_b[base:base + group, :TOK - 128] = out[p * group:(p + 1) * group, 128:]

    scaling = size ** -0.5
    lane = lax.broadcasted_iota(jnp.int32, (TOK, inner), 1) // size
    for w in range(wins):
        span = slice(w * TOK, (w + 1) * TOK)
        q, k, v, ga = proj[0, span], proj[1, span], proj[2, span], proj[3, span]
        sums = [None] * 4
        for h in range(heads):
            e = w * heads + h
            mine = (lane == h).astype(BF16)
            qh, kh, vh, gah = q * mine, k * mine, v * mine, ga * mine
            rows = pl.ds(e, TOK, stride=group)
            bias = jnp.concatenate([bias_a[rows, :], bias_b[rows, :][:, :TOK - 128]], axis=1)
            scores = dot(qh, k, NT) * scaling + bias
            top = jnp.max(scores, axis=1, keepdims=True)
            raised = jnp.exp(scores - top)
            soft = raised * (1.0 / jnp.sum(raised, axis=1, keepdims=True))
            half = soft.astype(BF16)
            grad_soft = dot(gah, v, NT)
            both = soft * grad_soft
            grad_scores = both - soft * jnp.sum(both, axis=1, keepdims=True)
            bias_a[rows, :] = grad_scores[:, :128]
            bias_b[rows, :] = jnp.concatenate(
                [grad_scores[:, 128:], jnp.zeros((TOK, 256 - TOK), F32)], axis=1
            )
            gsh = grad_scores.astype(BF16)
            terms = (dot(half, vh, NN), dot(gsh, kh, NN), dot(gsh, qh, TN), dot(half, gah, TN))
            sums = [t if s is None else s + t for s, t in zip(sums, terms)]
        att[span] = sums[0].astype(BF16)
        gproj[0, span] = (sums[1] * scaling).astype(BF16)
        gproj[1, span] = (sums[2] * scaling).astype(BF16)
        gproj[2, span] = sums[3].astype(BF16)

    chunks, chunk = piece_ref.shape[0], piece_ref.shape[-1]
    for n in range(chunks):
        cols = slice(n * chunk, (n + 1) * chunk)
        piece[:, :chunk] = sum(dot(gproj[c], aw_ref[c, cols, :], NT) for c in range(3))
        for c in range(WIN_LON):
            piece_ref[n, c] = piece[pl.ds(c, lines, stride=PAD), :][:, :chunk].astype(BF16)
    grad_w = [dot(gproj[c], tokens, TN).astype(BF16) for c in range(3)]
    grad_w.append(dot(att[...], grads, TN).astype(BF16))
    shares, share = grad_w_ref.shape[0], grad_w_ref.shape[1]
    grad_w = jnp.concatenate(grad_w, axis=0)
    for j in range(shares):
        grad_w_ref[j] = grad_w[j * share:(j + 1) * share]

    folded = jnp.zeros((ROWS * group, lanes), F32)
    for c in range(WIN_LON):
        place = lax.rem(c + WIN_LON - shift, WIN_LON)
        parts = []
        for p in range(ROWS):
            base = (p * PAD + c) * group
            parts.append(
                jnp.concatenate(
                    [bias_a[base:base + group, :], bias_b[base:base + group, :][:, :TOK - 128]], axis=1
                )
            )
        got = jnp.concatenate(parts, axis=0)
        one = got.astype(BF16)
        two = (got - one.astype(F32)).astype(BF16)
        folded = folded + pltpu.roll(dot(one, spread, NT) + dot(two, spread, NT), place, 1)
    rel[...] = folded.reshape(ROWS, group, lanes)
    for k in range(WIN_LEVEL * WIN_LEVEL * WIN_LAT):
        zi, zj, ai = k // (WIN_LEVEL * WIN_LAT), k // WIN_LAT % WIN_LEVEL, k % WIN_LAT
        line[:, k * part:(k + 1) * part] = rel[zi * WIN_LAT + ai, :, zj * part:(zj + 1) * part]
    strips, strip = grad_bias_ref.shape[0], grad_bias_ref.shape[2]
    for j in range(strips):
        grad_bias_ref[j] = line[:, j * strip:(j + 1) * strip].astype(BF16)


def block_backward(features, grad_out, low, high, attend_weight, output_weight, bias_table, bias_type, shift):
    levels, lat_rows, lon_cols, width = features.shape
    heads, rel_total = bias_table.shape[1:]
    inner = attend_weight.shape[2]
    wins = levels // WIN_LEVEL
    lines = wins * ROWS
    chunks = lax.axis_size("head")
    strips = lax.axis_size("lon")
    shares = strips * lax.axis_size("lat")
    strip = -(-rel_total // (128 * strips)) * 128
    vmem = pl.BlockSpec(memory_space=pltpu.VMEM)
    smem = pl.BlockSpec(memory_space=pltpu.SMEM)
    lanes = -(-ROWS * SPAN // 128) * 128
    total = lines * PAD
    return pl.pallas_call(
        functools.partial(block_kernel, heads),
        out_shape=(
            jax.ShapeDtypeStruct((chunks, WIN_LON, lines, width // chunks), BF16),
            jax.ShapeDtypeStruct((shares, 4 * inner // shares, width), BF16),
            jax.ShapeDtypeStruct((strips, PAD, strip), BF16),
            jax.ShapeDtypeStruct((PAD, 128), jnp.int32),
        ),
        in_specs=[smem, smem, vmem, vmem, vmem, vmem, vmem, vmem, pl.BlockSpec(memory_space=pl.ANY)],
        out_specs=(vmem, vmem, vmem, vmem),
        scratch_shapes=[
            pltpu.VMEM((total, width), BF16),
            pltpu.VMEM((total, width), BF16),
            pltpu.VMEM((4, total, inner), BF16),
            pltpu.VMEM((3, total, inner), BF16),
            pltpu.VMEM((total, inner), BF16),
            pltpu.VMEM((TOK * PAD, 128), F32),
            pltpu.VMEM((TOK * PAD, 128), F32),
            pltpu.VMEM((ROWS, PAD, lanes), F32),
            pltpu.VMEM((wins, heads, rel_total), F32),
            pltpu.VMEM((PAD, strips * strip), F32),
            pltpu.VMEM((total, 128), F32),
            pltpu.SemaphoreType.DMA((wins,)),
        ],
        compiler_params=pltpu.CompilerParams(vmem_limit_bytes=50 * 1024 * 1024),
        cost_estimate=pl.CostEstimate(flops=10**9, bytes_accessed=10**7, transcendentals=10**6),
    )(
        shift,
        bias_type,
        features.reshape(lines, lon_cols, width),
        grad_out.reshape(lines, lon_cols, width),
        low,
        high,
        attend_weight,
        output_weight,
        bias_table,
    )


def swap_columns(low, high, shift):
    if lax.axis_size("lon") <= 2:
        got = from_behind(jnp.where(shift <= HALF, low, high), "lon", 1)
        return got, got
    return from_behind(low, "lon", -1), from_behind(high, "lon", 1)


def exchange_kernel(shift_ref, piece_ref, w_ref, bias_ref, kinds_ref,
                    own_ref, edge_ref, all_w_ref, all_bias_ref, all_kinds_ref,
                    piece_in, w_in, bias_in, w_sum, bias_sum, edge_out, send, recv):
    lons, lats, heads = (lax.axis_size(name) for name in ("lon", "lat", "head"))
    lon, lat, head = (lax.axis_index(name) for name in ("lon", "lat", "head"))
    mine = lon * lats + lat
    pairs = [(a, b) for a in range(lons) for b in range(lats) if a or b]

    def grid_peer(a, b):
        return lax.rem(lon + a, lons), lax.rem(lat + b, lats)

    def group_peer(n):
        return lax.rem(head + n, heads)

    barrier = pltpu.get_barrier_semaphore()
    for a, b in pairs:
        x, y = grid_peer(a, b)
        pl.semaphore_signal(barrier, inc=1, device_id=(x, y, head), device_id_type=pl.DeviceIdType.MESH)
    for n in range(1, heads):
        pl.semaphore_signal(
            barrier, inc=1, device_id=(lon, lat, group_peer(n)), device_id_type=pl.DeviceIdType.MESH
        )
    pl.semaphore_wait(barrier, len(pairs) + heads - 1)
    count = [0]

    def post(src, dst, device):
        k = count[0]
        count[0] += 1
        copy = pltpu.make_async_remote_copy(
            src_ref=src, dst_ref=dst, send_sem=send.at[k], recv_sem=recv.at[k],
            device_id=device, device_id_type=pl.DeviceIdType.MESH,
        )
        copy.start()
        return copy

    bias_copies = []
    for a in range(1, lons):
        x, y = grid_peer(a, 0)
        bias_copies.append(post(bias_ref.at[x], bias_in.at[a - 1], (x, y, head)))
    w_copies = []
    for i, (a, b) in enumerate(pairs):
        x, y = grid_peer(a, b)
        w_copies.append(post(w_ref.at[x * lats + y], w_in.at[i], (x, y, head)))
    piece_copies = []
    for n in range(1, heads):
        to = group_peer(n)
        piece_copies.append(post(piece_ref.at[to], piece_in.at[n - 1], (lon, lat, to)))
    late = []
    for b in range(1, lats):
        x, y = grid_peer(0, b)
        late.append(post(kinds_ref, all_kinds_ref.at[lat], (x, y, head)))
    all_kinds_ref[pl.ds(lat, 1)] = kinds_ref[...][None]

    for copy in bias_copies:
        copy.wait_recv()
    total = bias_ref[lon].astype(F32)
    for a in range(lons - 1):
        total = total + bias_in[a].astype(F32)
    bias_sum[...] = total.astype(BF16)
    all_bias_ref[pl.ds(mine, 1)] = total.astype(BF16)[None]
    for a, b in pairs:
        x, y = grid_peer(a, b)
        late.append(post(bias_sum, all_bias_ref.at[mine], (x, y, head)))

    for copy in w_copies:
        copy.wait_recv()
    total = w_ref[mine].astype(F32)
    for i in range(len(pairs)):
        total = total + w_in[i].astype(F32)
    w_sum[...] = total.astype(BF16)
    all_w_ref[pl.ds(mine, 1)] = total.astype(BF16)[None]
    for a, b in pairs:
        x, y = grid_peer(a, b)
        late.append(post(w_sum, all_w_ref.at[mine], (x, y, head)))

    for copy in piece_copies:
        copy.wait_recv()
    total = piece_ref[head].astype(F32)
    for n in range(heads - 1):
        total = total + piece_in[n].astype(F32)
    own_ref[...] = total.astype(BF16)
    if lons <= 2:
        low = jnp.where(shift_ref[0] <= HALF, 1.0, 0.0)
        edge_out[:HALF] = (total[:HALF] * low + total[HALF:] * (1.0 - low)).astype(BF16)
    else:
        edge_out[...] = total.astype(BF16)
    sends = [(1, 0)] if lons <= 2 else [(1, 0), (lons - 1, HALF)]
    for a, first in sends:
        x, y = grid_peer(a, 0)
        late.append(post(edge_out.at[pl.ds(first, HALF)], edge_ref.at[pl.ds(first, HALF)], (x, y, head)))
    if lons <= 2:
        edge_ref[HALF:] = jnp.zeros_like(edge_out[HALF:])
    for copy in late:
        copy.wait_recv()
    for copy in bias_copies + w_copies + piece_copies + late:
        copy.wait_send()


def exchange(pieces, grad_w, grad_bias, kinds, shift):
    lons, lats, heads = (lax.axis_size(name) for name in ("lon", "lat", "head"))
    shares = lons * lats
    vmem = pl.BlockSpec(memory_space=pltpu.VMEM)
    copies = (lons - 1) + 3 * (shares - 1) + (heads - 1) + (lats - 1) + 2
    return pl.pallas_call(
        exchange_kernel,
        out_shape=(
            jax.ShapeDtypeStruct(pieces.shape[1:], BF16),
            jax.ShapeDtypeStruct(pieces.shape[1:], BF16),
            jax.ShapeDtypeStruct(grad_w.shape, BF16),
            jax.ShapeDtypeStruct((shares, *grad_bias.shape[1:]), BF16),
            jax.ShapeDtypeStruct((lats, *kinds.shape), jnp.int32),
        ),
        in_specs=[pl.BlockSpec(memory_space=pltpu.SMEM)] + [vmem] * 4,
        out_specs=(vmem,) * 5,
        scratch_shapes=[
            pltpu.VMEM((heads - 1, *pieces.shape[1:]), BF16),
            pltpu.VMEM((shares - 1, *grad_w.shape[1:]), BF16),
            pltpu.VMEM((max(lons - 1, 1), *grad_bias.shape[1:]), BF16),
            pltpu.VMEM(grad_w.shape[1:], BF16),
            pltpu.VMEM(grad_bias.shape[1:], BF16),
            pltpu.VMEM(pieces.shape[1:], BF16),
            pltpu.SemaphoreType.DMA((copies,)),
            pltpu.SemaphoreType.DMA((copies,)),
        ],
        compiler_params=pltpu.CompilerParams(
            collective_id=0, has_side_effects=True, vmem_limit_bytes=50 * 1024 * 1024
        ),
    )(shift, pieces, grad_w, grad_bias, kinds)


def finish_kernel(lats, shift_ref, own_ref, edge_ref, w_ref, bias_ref, kinds_ref,
                  feature_ref, aw_ref, ow_ref, table_ref, wide):
    shift = shift_ref[0]
    cols, lines, chunk = own_ref.shape
    for c in range(cols):
        flag = use_neighbour(shift, c).astype(F32)
        other = edge_ref[c % HALF] if lats[0] <= 2 else edge_ref[c]
        mixed = other.astype(F32) * flag + own_ref[c].astype(F32) * (1.0 - flag)
        wide[pl.ds(c, lines, stride=PAD), :] = jnp.concatenate(
            [mixed, jnp.zeros((lines, 128 - chunk), F32)], axis=1
        )
    feature_ref[...] = wide[...].reshape(lines, PAD, 128)[:, :cols, :chunk].astype(BF16)
    full = jnp.concatenate([w_ref[j].astype(F32) for j in range(w_ref.shape[0])], axis=0)
    inner = full.shape[0] // 4
    for c in range(3):
        aw_ref[c] = full[c * inner:(c + 1) * inner].T
    ow_ref[...] = full[3 * inner:]

    rows = kinds_ref.shape[0] * kinds_ref.shape[1]
    kinds = kinds_ref[...].reshape(rows, 128)
    types, heads, total = table_ref.shape
    held = lax.broadcasted_iota(jnp.int32, (rows, 128), 0) % kinds_ref.shape[1] % heads
    lane = lax.broadcasted_iota(jnp.int32, (rows, 128), 1)
    strip = bias_ref.shape[2]
    for h in range(heads):
        pick = ((kinds == lane) & (held == h)).astype(F32).astype(BF16)[:, :types]
        for j in range(lats[0]):
            wide_rows = jnp.concatenate(
                [bias_ref[j * lats[1] + b] for b in range(lats[1])], axis=0
            )
            stop = min(total, (j + 1) * strip)
            if stop > j * strip:
                out = dot(pick, wide_rows, TN)
                table_ref[:, h, j * strip:stop] = out[:, :stop - j * strip]


def finish(own, edge, all_w, all_bias, all_kinds, shift, types, heads, rel_total):
    cols, lines, chunk = own.shape
    inner = all_w.shape[0] * all_w.shape[1] // 4
    width = all_w.shape[2]
    vmem = pl.BlockSpec(memory_space=pltpu.VMEM)
    return pl.pallas_call(
        functools.partial(finish_kernel, (lax.axis_size("lon"), lax.axis_size("lat"))),
        out_shape=(
            jax.ShapeDtypeStruct((lines, cols, chunk), BF16),
            jax.ShapeDtypeStruct((3, width, inner), F32),
            jax.ShapeDtypeStruct((inner, width), F32),
            jax.ShapeDtypeStruct((types, heads, rel_total), F32),
        ),
        in_specs=[pl.BlockSpec(memory_space=pltpu.SMEM)] + [vmem] * 5,
        out_specs=(vmem,) * 4,
        scratch_shapes=[pltpu.VMEM((lines * PAD, 128), F32)],
        compiler_params=pltpu.CompilerParams(vmem_limit_bytes=50 * 1024 * 1024),
    )(shift, own, edge, all_w, all_bias, all_kinds)


def per_device(features, attend_weight, output_weight, bias_table, bias_type, window_shift, grad_out):
    shift = window_shift[0]
    levels, lat_rows, lon_cols, width = features.shape
    stacked = jnp.stack((features, grad_out)).reshape(2, levels * lat_rows, lon_cols, width)
    low, high = swap_columns(stacked[:, :, :HALF], stacked[:, :, HALF:], shift)
    pieces, grad_w, grad_bias, kinds = block_backward(
        features, grad_out, low, high, attend_weight, output_weight, bias_table, bias_type, window_shift
    )
    gathered = exchange(pieces, grad_w, grad_bias, kinds, window_shift)
    feature_grad, attend_grad, output_grad, bias_grad = finish(*gathered, window_shift, *bias_table.shape)
    return (feature_grad.reshape(levels, lat_rows, lon_cols, -1), attend_grad, output_grad, bias_grad)


def solution(mesh):
    placed = (
        P(None, "lat", "lon", None),
        P(None, None, "head"),
        P("head", None),
        P(None, "head", None),
        P(None, "lat"),
        P(),
        P(None, "lat", "lon", None),
    )
    return jax.shard_map(
        per_device,
        mesh=mesh,
        in_specs=placed,
        out_specs=(
            P(None, "lat", "lon", "head"),
            P(None, None, "head"),
            P("head", None),
            P(None, "head", None),
        ),
        check_vma=False,
    )
```

```python
import functools

import jax
import jax.numpy as jnp
from jax import lax
from jax.experimental import pallas as pl
from jax.experimental.pallas import tpu as pltpu
from jax.sharding import PartitionSpec as P

WIN_LEVEL = 2
WIN_LAT = 6
WIN_LON = 12
ROWS = WIN_LEVEL * WIN_LAT
HALF = WIN_LON // 2
SPAN = 2 * WIN_LON - 1
PAD = 16
TOK = ROWS * PAD
F32 = jnp.float32
BF16 = jnp.bfloat16


def from_behind(x, axis, by):
    count = lax.axis_size(axis)
    return lax.ppermute(x, axis, [(i, (i + by) % count) for i in range(count)])


def dot(a, b, dims):
    return lax.dot_general(a, b, (dims, ((), ())), preferred_element_type=F32)


NN = ((1,), (0,))
NT = ((1,), (1,))
TN = ((0,), (0,))


def use_neighbour(shift, col):
    first = jnp.where(shift <= HALF, 0, shift)
    return (col >= first) & (col < jnp.where(shift <= HALF, shift, WIN_LON))


def spread_matrix(lanes, shift):
    row = lax.broadcasted_iota(jnp.int32, (lanes, TOK), 0)
    key = lax.broadcasted_iota(jnp.int32, (lanes, TOK), 1)
    slot = key % PAD
    pos = slot + WIN_LON - shift
    pos = jnp.where(pos >= WIN_LON, pos - WIN_LON, pos)
    hit = (row == key // PAD * SPAN + WIN_LON - 1 - pos) & (slot < WIN_LON)
    return jnp.where(hit, 1.0, 0.0).astype(BF16)


def bias_kernel(heads, shift_ref, type_ref, table_ref, bias_a, bias_b, kinds_ref, rel, table, line, sems):
    shift = shift_ref[0]
    wins = table.shape[0]
    part = WIN_LAT * SPAN
    copies = [
        pltpu.make_async_copy(table_ref.at[type_ref[w, 0]], table.at[w], sems.at[w]) for w in range(wins)
    ]
    for copy in copies:
        copy.start()

    for copy in copies:
        copy.wait()
    rel[...] = jnp.zeros_like(rel)
    line[...] = jnp.zeros_like(line)
    kinds_ref[...] = jnp.full_like(kinds_ref, -1)
    for w in range(wins):
        line[w * heads:(w + 1) * heads, :table.shape[2]] = table[w]
        kinds_ref[w * heads:(w + 1) * heads, :] = jnp.full((heads, kinds_ref.shape[1]), type_ref[w, 0], jnp.int32)
    for k in range(WIN_LEVEL * WIN_LEVEL * WIN_LAT):
        zi, zj, ai = k // (WIN_LEVEL * WIN_LAT), k // WIN_LAT % WIN_LEVEL, k % WIN_LAT
        rel[zi * WIN_LAT + ai, :, zj * part:(zj + 1) * part] = line[:, k * part:(k + 1) * part]
    lanes = rel.shape[2]
    spread = spread_matrix(lanes, shift)
    unused = jnp.where(lax.broadcasted_iota(jnp.int32, (1, TOK), 1) % PAD < WIN_LON, 0.0, -1e30)
    group = PAD
    flat = rel[...].reshape(ROWS * group, lanes)
    for c in range(PAD):
        if c < WIN_LON:
            place = lax.rem(c + WIN_LON - shift, WIN_LON)
            moved = pltpu.roll(flat, lanes - place, 1)
            one = moved.astype(BF16)
            rest = moved - one.astype(F32)
            two = rest.astype(BF16)
            three = (rest - two.astype(F32)).astype(BF16)
            out = dot(one, spread, NN) + dot(two, spread, NN) + dot(three, spread, NN) + unused
        else:
            out = jnp.zeros((ROWS * group, TOK), F32)
        for p in range(ROWS):
            base = (p * PAD + c) * group
            bias_a[base:base + group, :] = out[p * group:(p + 1) * group, :128]
            bias_b[base:base + group, :TOK - 128] = out[p * group:(p + 1) * group, 128:]


def spread_bias(bias_table, bias_type, shift):
    heads, rel_total = bias_table.shape[1:]
    wins = bias_type.shape[0]
    vmem = pl.BlockSpec(memory_space=pltpu.VMEM)
    smem = pl.BlockSpec(memory_space=pltpu.SMEM)
    lanes = -(-ROWS * SPAN // 128) * 128
    return pl.pallas_call(
        functools.partial(bias_kernel, heads),
        out_shape=(
            jax.ShapeDtypeStruct((TOK * PAD, 128), F32),
            jax.ShapeDtypeStruct((TOK * PAD, 128), F32),
            jax.ShapeDtypeStruct((PAD, 128), jnp.int32),
        ),
        in_specs=[smem, smem, pl.BlockSpec(memory_space=pl.ANY)],
        out_specs=(vmem,) * 3,
        scratch_shapes=[
            pltpu.VMEM((ROWS, PAD, lanes), F32),
            pltpu.VMEM((wins, heads, rel_total), F32),
            pltpu.VMEM((PAD, -(-rel_total // 128) * 128), F32),
            pltpu.SemaphoreType.DMA((wins,)),
        ],
        compiler_params=pltpu.CompilerParams(vmem_limit_bytes=20 * 1024 * 1024),
        cost_estimate=pl.CostEstimate(flops=5 * 10**8, bytes_accessed=4 * 10**6, transcendentals=0),
    )(shift, bias_type, bias_table)


def block_kernel(heads, shift_ref, x_ref, g_ref, low_ref, high_ref, aw_ref, ow_ref, from_a, from_b,
                 piece_ref, grad_w_ref, grad_bias_ref,
                 xs, gs, proj, gproj, att, bias_a, bias_b, rel, line, piece):
    shift = shift_ref[0]
    wins = x_ref.shape[0] // ROWS
    width = x_ref.shape[-1]
    inner = aw_ref.shape[2]
    size = inner // heads
    part = WIN_LAT * SPAN
    lines = wins * ROWS
    col = lax.broadcasted_iota(jnp.int32, (lines, WIN_LON, width), 1)
    taken = use_neighbour(shift, col)
    for src, dst, n in ((x_ref, xs, 0), (g_ref, gs, 1)):
        near = jnp.concatenate([low_ref[n].astype(F32), high_ref[n].astype(F32)], axis=1)
        picked = jnp.where(taken, near, src[...].astype(F32))
        full = jnp.concatenate([picked, jnp.zeros((lines, PAD - WIN_LON, width), F32)], axis=1)
        dst[...] = full.astype(BF16).reshape(lines * PAD, width)
    tokens = xs[...]
    grads = gs[...]
    for c in range(3):
        proj[c] = dot(tokens, aw_ref[c], NN).astype(BF16)
    proj[3] = dot(grads, ow_ref[...], NT).astype(BF16)

    spread = spread_matrix(rel.shape[2], shift)
    lanes = rel.shape[2]
    group = PAD

    scaling = size ** -0.5
    lane = lax.broadcasted_iota(jnp.int32, (TOK, inner), 1) // size
    for w in range(wins):
        span = slice(w * TOK, (w + 1) * TOK)
        q, k, v, ga = proj[0, span], proj[1, span], proj[2, span], proj[3, span]
        sums = [None] * 4
        for h in range(heads):
            e = w * heads + h
            mine = (lane == h).astype(BF16)
            qh, kh, vh, gah = q * mine, k * mine, v * mine, ga * mine
            rows = pl.ds(e, TOK, stride=group)
            bias = jnp.concatenate([from_a[rows, :], from_b[rows, :][:, :TOK - 128]], axis=1)
            scores = dot(qh, k, NT) * scaling + bias
            top = jnp.max(scores, axis=1, keepdims=True)
            raised = jnp.exp(scores - top)
            soft = raised * (1.0 / jnp.sum(raised, axis=1, keepdims=True))
            half = soft.astype(BF16)
            grad_soft = dot(gah, v, NT)
            both = soft * grad_soft
            grad_scores = both - soft * jnp.sum(both, axis=1, keepdims=True)
            bias_a[rows, :] = grad_scores[:, :128]
            bias_b[rows, :] = jnp.concatenate(
                [grad_scores[:, 128:], jnp.zeros((TOK, 256 - TOK), F32)], axis=1
            )
            gsh = grad_scores.astype(BF16)
            terms = (dot(half, vh, NN), dot(gsh, kh, NN), dot(gsh, qh, TN), dot(half, gah, TN))
            sums = [t if s is None else s + t for s, t in zip(sums, terms)]
        att[span] = sums[0].astype(BF16)
        gproj[0, span] = (sums[1] * scaling).astype(BF16)
        gproj[1, span] = (sums[2] * scaling).astype(BF16)
        gproj[2, span] = sums[3].astype(BF16)

    chunks, chunk = piece_ref.shape[0], piece_ref.shape[-1]
    for n in range(chunks):
        cols = slice(n * chunk, (n + 1) * chunk)
        piece[:, :chunk] = sum(dot(gproj[c], aw_ref[c, cols, :], NT) for c in range(3))
        for c in range(WIN_LON):
            piece_ref[n, c] = piece[pl.ds(c, lines, stride=PAD), :][:, :chunk].astype(BF16)
    grad_w = [dot(gproj[c], tokens, TN).astype(BF16) for c in range(3)]
    grad_w.append(dot(att[...], grads, TN).astype(BF16))
    shares, share = grad_w_ref.shape[0], grad_w_ref.shape[1]
    grad_w = jnp.concatenate(grad_w, axis=0)
    for j in range(shares):
        grad_w_ref[j] = grad_w[j * share:(j + 1) * share]

    line[...] = jnp.zeros_like(line)
    folded = jnp.zeros((ROWS * group, lanes), F32)
    for c in range(WIN_LON):
        place = lax.rem(c + WIN_LON - shift, WIN_LON)
        parts = []
        for p in range(ROWS):
            base = (p * PAD + c) * group
            parts.append(
                jnp.concatenate(
                    [bias_a[base:base + group, :], bias_b[base:base + group, :][:, :TOK - 128]], axis=1
                )
            )
        got = jnp.concatenate(parts, axis=0)
        one = got.astype(BF16)
        two = (got - one.astype(F32)).astype(BF16)
        folded = folded + pltpu.roll(dot(one, spread, NT) + dot(two, spread, NT), place, 1)
    rel[...] = folded.reshape(ROWS, group, lanes)
    for k in range(WIN_LEVEL * WIN_LEVEL * WIN_LAT):
        zi, zj, ai = k // (WIN_LEVEL * WIN_LAT), k // WIN_LAT % WIN_LEVEL, k % WIN_LAT
        line[:, k * part:(k + 1) * part] = rel[zi * WIN_LAT + ai, :, zj * part:(zj + 1) * part]
    strips, strip = grad_bias_ref.shape[0], grad_bias_ref.shape[2]
    for j in range(strips):
        used = lax.broadcasted_iota(jnp.int32, (PAD, strip), 0) < wins * heads
        grad_bias_ref[j] = jnp.where(used, line[:, j * strip:(j + 1) * strip], 0.0).astype(BF16)


def block_backward(features, grad_out, low, high, attend_weight, output_weight, bias, table_shape, shift):
    levels, lat_rows, lon_cols, width = features.shape
    heads, rel_total = table_shape[1:]
    inner = attend_weight.shape[2]
    wins = levels // WIN_LEVEL
    lines = wins * ROWS
    chunks = lax.axis_size("head")
    strips = lax.axis_size("lon")
    shares = strips * lax.axis_size("lat")
    strip = -(-rel_total // (128 * strips)) * 128
    vmem = pl.BlockSpec(memory_space=pltpu.VMEM)
    smem = pl.BlockSpec(memory_space=pltpu.SMEM)
    lanes = -(-ROWS * SPAN // 128) * 128
    total = lines * PAD
    return pl.pallas_call(
        functools.partial(block_kernel, heads),
        out_shape=(
            jax.ShapeDtypeStruct((chunks, WIN_LON, lines, width // chunks), BF16),
            jax.ShapeDtypeStruct((shares, 4 * inner // shares, width), BF16),
            jax.ShapeDtypeStruct((strips, PAD, strip), BF16),
        ),
        in_specs=[smem] + [vmem] * 8,
        out_specs=(vmem,) * 3,
        scratch_shapes=[
            pltpu.VMEM((total, width), BF16),
            pltpu.VMEM((total, width), BF16),
            pltpu.VMEM((4, total, inner), BF16),
            pltpu.VMEM((3, total, inner), BF16),
            pltpu.VMEM((total, inner), BF16),
            pltpu.VMEM((TOK * PAD, 128), F32),
            pltpu.VMEM((TOK * PAD, 128), F32),
            pltpu.VMEM((ROWS, PAD, lanes), F32),
            pltpu.VMEM((PAD, strips * strip), F32),
            pltpu.VMEM((total, 128), F32),
        ],
        compiler_params=pltpu.CompilerParams(vmem_limit_bytes=50 * 1024 * 1024),
        cost_estimate=pl.CostEstimate(flops=10**9, bytes_accessed=10**7, transcendentals=10**6),
    )(
        shift,
        features.reshape(lines, lon_cols, width),
        grad_out.reshape(lines, lon_cols, width),
        low,
        high,
        attend_weight,
        output_weight,
        *bias,
    )


def swap_columns(low, high, shift):
    if lax.axis_size("lon") <= 2:
        got = from_behind(jnp.where(shift <= HALF, low, high), "lon", 1)
        return got, got
    return from_behind(low, "lon", -1), from_behind(high, "lon", 1)


def exchange_kernel(shift_ref, piece_ref, w_ref, bias_ref, kinds_ref,
                    own_ref, edge_ref, all_w_ref, all_bias_ref, all_kinds_ref,
                    piece_in, w_in, bias_in, w_sum, bias_sum, edge_out, send, recv):
    lons, lats, heads = (lax.axis_size(name) for name in ("lon", "lat", "head"))
    lon, lat, head = (lax.axis_index(name) for name in ("lon", "lat", "head"))
    mine = lon * lats + lat
    pairs = [(a, b) for a in range(lons) for b in range(lats) if a or b]

    def grid_peer(a, b):
        return lax.rem(lon + a, lons), lax.rem(lat + b, lats)

    def group_peer(n):
        return lax.rem(head + n, heads)

    barrier = pltpu.get_barrier_semaphore()
    for a, b in pairs:
        x, y = grid_peer(a, b)
        pl.semaphore_signal(barrier, inc=1, device_id=(x, y, head), device_id_type=pl.DeviceIdType.MESH)
    for n in range(1, heads):
        pl.semaphore_signal(
            barrier, inc=1, device_id=(lon, lat, group_peer(n)), device_id_type=pl.DeviceIdType.MESH
        )
    pl.semaphore_wait(barrier, len(pairs) + heads - 1)
    count = [0]

    def post(src, dst, device):
        k = count[0]
        count[0] += 1
        copy = pltpu.make_async_remote_copy(
            src_ref=src, dst_ref=dst, send_sem=send.at[k], recv_sem=recv.at[k],
            device_id=device, device_id_type=pl.DeviceIdType.MESH,
        )
        copy.start()
        return copy

    bias_copies = []
    for a in range(1, lons):
        x, y = grid_peer(a, 0)
        bias_copies.append(post(bias_ref.at[x], bias_in.at[a - 1], (x, y, head)))
    w_copies = []
    for i, (a, b) in enumerate(pairs):
        x, y = grid_peer(a, b)
        w_copies.append(post(w_ref.at[x * lats + y], w_in.at[i], (x, y, head)))
    piece_copies = []
    for n in range(1, heads):
        to = group_peer(n)
        piece_copies.append(post(piece_ref.at[to], piece_in.at[n - 1], (lon, lat, to)))
    late = []
    for b in range(1, lats):
        x, y = grid_peer(0, b)
        late.append(post(kinds_ref, all_kinds_ref.at[lat], (x, y, head)))
    all_kinds_ref[pl.ds(lat, 1)] = kinds_ref[...][None]

    for copy in bias_copies:
        copy.wait_recv()
    total = bias_ref[lon].astype(F32)
    for a in range(lons - 1):
        total = total + bias_in[a].astype(F32)
    bias_sum[...] = total.astype(BF16)
    all_bias_ref[pl.ds(mine, 1)] = total.astype(BF16)[None]
    for a, b in pairs:
        x, y = grid_peer(a, b)
        late.append(post(bias_sum, all_bias_ref.at[mine], (x, y, head)))

    for copy in w_copies:
        copy.wait_recv()
    total = w_ref[mine].astype(F32)
    for i in range(len(pairs)):
        total = total + w_in[i].astype(F32)
    w_sum[...] = total.astype(BF16)
    all_w_ref[pl.ds(mine, 1)] = total.astype(BF16)[None]
    for a, b in pairs:
        x, y = grid_peer(a, b)
        late.append(post(w_sum, all_w_ref.at[mine], (x, y, head)))

    for copy in piece_copies:
        copy.wait_recv()
    total = piece_ref[head].astype(F32)
    for n in range(heads - 1):
        total = total + piece_in[n].astype(F32)
    own_ref[...] = total.astype(BF16)
    if lons <= 2:
        low = jnp.where(shift_ref[0] <= HALF, 1.0, 0.0)
        edge_out[:HALF] = (total[:HALF] * low + total[HALF:] * (1.0 - low)).astype(BF16)
    else:
        edge_out[...] = total.astype(BF16)
    sends = [(1, 0)] if lons <= 2 else [(1, 0), (lons - 1, HALF)]
    for a, first in sends:
        x, y = grid_peer(a, 0)
        late.append(post(edge_out.at[pl.ds(first, HALF)], edge_ref.at[pl.ds(first, HALF)], (x, y, head)))
    if lons <= 2:
        edge_ref[HALF:] = jnp.zeros_like(edge_out[HALF:])
    for copy in late:
        copy.wait_recv()
    for copy in bias_copies + w_copies + piece_copies + late:
        copy.wait_send()


def exchange(pieces, grad_w, grad_bias, kinds, shift):
    lons, lats, heads = (lax.axis_size(name) for name in ("lon", "lat", "head"))
    shares = lons * lats
    vmem = pl.BlockSpec(memory_space=pltpu.VMEM)
    copies = (lons - 1) + 3 * (shares - 1) + (heads - 1) + (lats - 1) + 2
    return pl.pallas_call(
        exchange_kernel,
        out_shape=(
            jax.ShapeDtypeStruct(pieces.shape[1:], BF16),
            jax.ShapeDtypeStruct(pieces.shape[1:], BF16),
            jax.ShapeDtypeStruct(grad_w.shape, BF16),
            jax.ShapeDtypeStruct((shares, *grad_bias.shape[1:]), BF16),
            jax.ShapeDtypeStruct((lats, *kinds.shape), jnp.int32),
        ),
        in_specs=[pl.BlockSpec(memory_space=pltpu.SMEM)] + [vmem] * 4,
        out_specs=(vmem,) * 5,
        scratch_shapes=[
            pltpu.VMEM((heads - 1, *pieces.shape[1:]), BF16),
            pltpu.VMEM((shares - 1, *grad_w.shape[1:]), BF16),
            pltpu.VMEM((max(lons - 1, 1), *grad_bias.shape[1:]), BF16),
            pltpu.VMEM(grad_w.shape[1:], BF16),
            pltpu.VMEM(grad_bias.shape[1:], BF16),
            pltpu.VMEM(pieces.shape[1:], BF16),
            pltpu.SemaphoreType.DMA((copies,)),
            pltpu.SemaphoreType.DMA((copies,)),
        ],
        compiler_params=pltpu.CompilerParams(
            collective_id=0, has_side_effects=True, vmem_limit_bytes=50 * 1024 * 1024
        ),
    )(shift, pieces, grad_w, grad_bias, kinds)


def finish_kernel(lats, shift_ref, own_ref, edge_ref, w_ref, bias_ref, kinds_ref,
                  feature_ref, aw_ref, ow_ref, table_ref, wide):
    shift = shift_ref[0]
    cols, lines, chunk = own_ref.shape
    for c in range(cols):
        flag = use_neighbour(shift, c).astype(F32)
        other = edge_ref[c % HALF] if lats[0] <= 2 else edge_ref[c]
        mixed = other.astype(F32) * flag + own_ref[c].astype(F32) * (1.0 - flag)
        wide[c * lines:(c + 1) * lines, :chunk] = mixed
        for a in range(WIN_LAT):
            levels = wide[pl.ds(c * lines + a, lines // WIN_LAT, stride=WIN_LAT), :]
            feature_ref[a, c] = levels[:, :chunk].astype(BF16)
    full = jnp.concatenate([w_ref[j].astype(F32) for j in range(w_ref.shape[0])], axis=0)
    inner = full.shape[0] // 4
    for c in range(3):
        aw_ref[c] = full[c * inner:(c + 1) * inner]
    ow_ref[...] = full[3 * inner:]

    rows = kinds_ref.shape[0] * kinds_ref.shape[1]
    kinds = kinds_ref[...].reshape(rows, 128)
    heads, types, total = table_ref.shape
    held = lax.broadcasted_iota(jnp.int32, (rows, 128), 0) % kinds_ref.shape[1] % heads
    lane = lax.broadcasted_iota(jnp.int32, (rows, 128), 1)
    strip = bias_ref.shape[2]
    for h in range(heads):
        pick = ((kinds == lane) & (held == h)).astype(F32).astype(BF16)[:, :types]
        for j in range(lats[0]):
            wide_rows = jnp.concatenate(
                [bias_ref[j * lats[1] + b] for b in range(lats[1])], axis=0
            )
            stop = min(total, (j + 1) * strip)
            if stop > j * strip:
                out = dot(pick, wide_rows, TN)
                table_ref[h, :, j * strip:stop] = out[:, :stop - j * strip]


def finish(own, edge, all_w, all_bias, all_kinds, shift, types, heads, rel_total):
    cols, lines, chunk = own.shape
    inner = all_w.shape[0] * all_w.shape[1] // 4
    width = all_w.shape[2]
    vmem = pl.BlockSpec(memory_space=pltpu.VMEM)
    return pl.pallas_call(
        functools.partial(finish_kernel, (lax.axis_size("lon"), lax.axis_size("lat"))),
        out_shape=(
            jax.ShapeDtypeStruct((WIN_LAT, cols, lines // WIN_LAT, chunk), BF16),
            jax.ShapeDtypeStruct((3, inner, width), F32),
            jax.ShapeDtypeStruct((inner, width), F32),
            jax.ShapeDtypeStruct((heads, types, rel_total), F32),
        ),
        in_specs=[pl.BlockSpec(memory_space=pltpu.SMEM)] + [vmem] * 5,
        out_specs=(vmem,) * 4,
        scratch_shapes=[pltpu.VMEM((lines * cols, 128), F32)],
        compiler_params=pltpu.CompilerParams(vmem_limit_bytes=50 * 1024 * 1024),
    )(shift, own, edge, all_w, all_bias, all_kinds)


def per_device(features, attend_weight, output_weight, bias_table, bias_type, window_shift, grad_out):
    shift = window_shift[0]
    levels, lat_rows, lon_cols, width = features.shape
    stored = [x.transpose(1, 2, 0, 3) for x in (features, grad_out)]
    low, high = swap_columns(
        jnp.stack([x[:, :HALF] for x in stored]), jnp.stack([x[:, HALF:] for x in stored]), shift
    )
    bias = spread_bias(bias_table, bias_type, window_shift)
    low, high = (
        x.transpose(0, 3, 1, 2, 4).reshape(2, levels * lat_rows, HALF, width) for x in (low, high)
    )
    pieces, grad_w, grad_bias = block_backward(
        features, grad_out, low, high, attend_weight, output_weight, bias[:2], bias_table.shape, window_shift
    )
    kinds = bias[2]
    gathered = exchange(pieces, grad_w, grad_bias, kinds, window_shift)
    feature_grad, attend_grad, output_grad, bias_grad = finish(*gathered, window_shift, *bias_table.shape)
    return (
        feature_grad.transpose(2, 0, 1, 3),
        attend_grad.transpose(0, 2, 1),
        output_grad,
        bias_grad.transpose(1, 0, 2),
    )


def solution(mesh):
    placed = (
        P(None, "lat", "lon", None),
        P(None, None, "head"),
        P("head", None),
        P(None, "head", None),
        P(None, "lat"),
        P(),
        P(None, "lat", "lon", None),
    )
    return jax.shard_map(
        per_device,
        mesh=mesh,
        in_specs=placed,
        out_specs=(
            P(None, "lat", "lon", "head"),
            P(None, None, "head"),
            P("head", None),
            P(None, "head", None),
        ),
        check_vma=False,
    )
```
